32 devices in a mesh: groups: 2 (over x), sp: 8 (over z, y), fsdp: 2 (over core).
Axes of the slice: x: 2, y: 2, z: 4, core: 2. Of those that a mesh axis runs over, the one named last changes fastest.
Arguments:
- policy_hidden: bfloat16 [4, 256, 4096], P(('groups', 'fsdp'), 'sp'), parts along dimension 0, may hold values from -6 to 6
- policy_queries: bfloat16 [4, 256, 1024], P(('groups', 'fsdp'), 'sp'), parts along dimension 0, may hold values from -512 to 512
- policy_documents: int32 [4, 256], P(('groups', 'fsdp'), 'sp'), parts along dimension 0, may hold values from 0 to 31, never falling along the last dimension, each value on 1 to 128 neighbouring positions
- policy_gain: bfloat16 [4096], P(('sp', 'fsdp')), may hold values from 0.099609375 to 1.8984375
- policy_key_weight: bfloat16 [4096, 512], P(('sp', 'fsdp')), may hold values from -0.09375 to 0.09375
- policy_value_weight: bfloat16 [4096, 512], P(('sp', 'fsdp')), may hold values from -0.09375 to 0.09375
- frozen_hidden: bfloat16 [4, 256, 4096], P(('groups', 'fsdp'), 'sp'), parts along dimension 0, may hold values from -6 to 6
- frozen_queries: bfloat16 [4, 256, 1024], P(('groups', 'fsdp'), 'sp'), parts along dimension 0, may hold values from -512 to 512
- frozen_documents: int32 [4, 256], P(('groups', 'fsdp'), 'sp'), parts along dimension 0, may hold values from 0 to 31, never falling along the last dimension, each value on 1 to 128 neighbouring positions
- frozen_gain: bfloat16 [4096], P(('sp', 'fsdp')), may hold values from 0.099609375 to 1.8984375
- frozen_key_weight: bfloat16 [4096, 512], P(('sp', 'fsdp')), may hold values from -0.09375 to 0.09375
- frozen_value_weight: bfloat16 [4096, 512], P(('sp', 'fsdp')), may hold values from -0.09375 to 0.09375
Outputs:
- policy_mixed: bfloat16 [4, 256, 1024], P(('groups', 'fsdp'), 'sp'), parts along dimension 0
- frozen_mixed: bfloat16 [4, 256, 1024], P(('groups', 'fsdp'), 'sp'), parts along dimension 0
The draws below stay inside these ranges and needn't reach their ends.
There are 2 independent parts, one for each index of `groups`. The reference program is written for one: setup_inputs(seed, part) draws one part's arguments, and reference() takes and returns one part's arrays. A program takes and returns all parts, laid end to end along the dimension named above; an argument that names none is the same for every part. Nothing has to cross between parts.
Inputs may be any that keep to these rules, and one draw needn't show every extreme that they name: `policy_documents`: along each sequence the ids never fall, and each document holds 1 to 128 positions. `frozen_documents`: along each sequence the ids never fall, and each document holds 1 to 128 positions.
All inputs are finite; a program needn't handle non-finite values.
Results may differ from the reference program's by a relative error of at most 0.007.
The reference program's roundings to bfloat16 on the way count: a program that leaves them out, or rounds other values in their place, can miss the bound.
Values may be sent and summed in bfloat16 or wider, within the bound.
No kernel may reach another device: no remote copies, remote signals or barrier semaphores. Data moves between devices by JAX's collectives and lax.ppermute only.
A program may use at most 128 MiB of HBM per device.

```python
import math
import jax
import jax.numpy as jnp
import numpy as np
from jax import lax

D = 4096
HEAD_DIM = 128
KV_HEADS = 4
DOCS = 32
HEADS = 8
LENGTH = 256
DOC_MOST = 128
SEQS = 2


def query_draw(seed_key):
    standard = jax.random.normal(seed_key, (SEQS, LENGTH, HEADS, HEAD_DIM), jnp.float32)
    drawn = 2.5 * standard
    return jnp.clip(drawn, -512.0, 512.0).reshape(SEQS, LENGTH, HEADS * HEAD_DIM).astype(jnp.bfloat16)


def draw_policy_queries(key, part):
    return query_draw(jax.random.fold_in(key, 11))


def draw_frozen_queries(key, part):
    return query_draw(jax.random.fold_in(key, 23))


def levels(stream_key, dims, pieces, least, high):
    level, own = 1.0, jax.random.fold_in(stream_key, 6)
    for dim, blocks in pieces:
        steps = jnp.exp(jax.random.uniform(jax.random.fold_in(own, dim), (blocks,), jnp.float32, least / len(pieces), high / len(pieces)))
        level = level * jnp.repeat(steps, dims[dim] // blocks).reshape([-1 if axis == dim else 1 for axis in range(len(dims))])
    return level


def split_up(amount, total, limit, skew):
    portions = [(1 << 20) // math.isqrt(rank ** skew) + 1 for rank in range(2, amount + 1)]
    rest, counts = total - limit - (amount - 1), [1] * (amount - 1)
    while rest > 0:
        movable = [i for i in range(amount - 1) if counts[i] < limit]
        whole, budget = sum([portions[i] for i in movable]), rest
        for i in movable:
            extra = min(limit - counts[i], max(1, budget * portions[i] // whole), rest)
            counts[i] = counts[i] + extra
            rest = rest - extra
    return np.array([limit] + counts)


def ragged_sizes(own_key, count, total, bound, skew):
    if count == 2:
        one = jax.random.randint(own_key, (), max(1, total - bound), min(bound, total - 1) + 1)
        return jnp.stack([one, total - one])
    sizes = jnp.asarray(split_up(count, total, bound, skew), jnp.int32)
    pairs = (count - 1) // 2
    donor, sink = sizes[1:1 + 2 * pairs:2], sizes[2:2 + 2 * pairs:2]
    room = jnp.minimum(donor - 1, bound - sink)
    moved = jax.random.randint(jax.random.fold_in(own_key, 1), (pairs,), 0, 1 << 20) % (room + 1)
    sizes = sizes.at[1:1 + 2 * pairs:2].set(donor - moved).at[2:2 + 2 * pairs:2].set(sink + moved)
    return sizes[jax.random.permutation(jax.random.fold_in(own_key, 2), count)]


def bell_draw(key, shape, scale, reach, shards=(), kind=jnp.bfloat16):
    entries = scale * jax.random.normal(key, shape, jnp.float32)
    if shards:
        entries = entries * levels(key, shape, shards, -0.22, 0.18)
    return jnp.clip(entries, -reach, reach).astype(kind)


def setup_inputs(seed: int = 0, part: int = 0) -> dict:
    seeds = jax.random.split(jax.random.key(seed), 13)
    part_keys = jax.random.split(jax.random.fold_in(seeds[12], part), 13)
    policy_hidden = bell_draw(part_keys[0], (SEQS, LENGTH, D), 1.0, 6.0, ((0, 2), (1, 8)))
    policy_queries = draw_policy_queries(jax.random.fold_in(jax.random.fold_in(seeds[12], part), 71), part)
    policy_documents = jax.vmap(lambda own: jnp.searchsorted(jnp.cumsum(ragged_sizes(own, DOCS, LENGTH, DOC_MOST, 1)), jnp.arange(LENGTH), side="right"))(jax.random.split(part_keys[2], SEQS)).reshape((SEQS, LENGTH)).astype(jnp.int32)
    policy_gain = jnp.clip(1.0 + 0.18 * jax.random.normal(seeds[3], (D,), jnp.float32), 0.099609375, 1.8984375).astype(jnp.bfloat16)
    policy_key_weight = bell_draw(seeds[4], (D, KV_HEADS * HEAD_DIM), D ** -0.5, 0.09375, ((0, 16),))
    policy_value_weight = bell_draw(seeds[5], (D, KV_HEADS * HEAD_DIM), D ** -0.5, 0.09375, ((0, 16),))
    frozen_hidden = bell_draw(part_keys[6], (SEQS, LENGTH, D), 1.0, 6.0, ((0, 2), (1, 8)))
    frozen_queries = draw_frozen_queries(jax.random.fold_in(jax.random.fold_in(seeds[12], part), 71), part)
    frozen_documents = jax.vmap(lambda own: jnp.searchsorted(jnp.cumsum(ragged_sizes(own, DOCS, LENGTH, DOC_MOST, 1)), jnp.arange(LENGTH), side="right"))(jax.random.split(part_keys[8], SEQS)).reshape((SEQS, LENGTH)).astype(jnp.int32)
    frozen_gain = jnp.clip(1.0 + 0.18 * jax.random.normal(seeds[9], (D,), jnp.float32), 0.099609375, 1.8984375).astype(jnp.bfloat16)
    frozen_key_weight = bell_draw(seeds[10], (D, KV_HEADS * HEAD_DIM), D ** -0.5, 0.09375, ((0, 16),))
    frozen_value_weight = bell_draw(seeds[11], (D, KV_HEADS * HEAD_DIM), D ** -0.5, 0.09375, ((0, 16),))
    return {"policy_hidden": policy_hidden, "policy_queries": policy_queries, "policy_documents": policy_documents, "policy_gain": policy_gain, "policy_key_weight": policy_key_weight, "policy_value_weight": policy_value_weight, "frozen_hidden": frozen_hidden, "frozen_queries": frozen_queries, "frozen_documents": frozen_documents, "frozen_gain": frozen_gain, "frozen_key_weight": frozen_key_weight, "frozen_value_weight": frozen_value_weight}


EPS = 1e-05
ROPE_BASE = 500000.0
MASKED = -1e+30

def rotate(raw_keys, positions):
    half_dim = HEAD_DIM // 2
    frequency = jnp.exp(-jnp.log(ROPE_BASE) * jnp.arange(half_dim, dtype=jnp.float32) * 2.0 / HEAD_DIM)
    angles = positions.astype(jnp.float32)[:, None] * frequency[None, :]
    cosines = jnp.cos(angles)[:, None, :]
    sines = jnp.sin(angles)[:, None, :]
    front_half = raw_keys[..., :half_dim]
    back_half = raw_keys[..., half_dim:]
    return jnp.concatenate([front_half * cosines - back_half * sines, back_half * cosines + front_half * sines], axis=-1)

def one_model(hidden, queries, documents, gain, key_weight, value_weight):
    group_size = HEADS // KV_HEADS
    factor = HEAD_DIM ** (-0.5)
    block_rows = min(512, LENGTH)
    margin = min(512, LENGTH // 2)
    window = block_rows + margin

    def one_sequence(inputs):
        sequence, query_rows, doc_row = inputs
        widened = sequence.astype(jnp.float32)
        inverse = lax.rsqrt(lax.optimization_barrier(jnp.mean(widened * widened, axis=-1, keepdims=True)) + EPS)
        normed = (widened * inverse * gain.astype(jnp.float32)[None, :]).astype(jnp.bfloat16)
        positions = jnp.arange(LENGTH, dtype=jnp.int32)
        raw_keys = jnp.dot(normed, key_weight, preferred_element_type=jnp.float32).reshape(LENGTH, KV_HEADS, HEAD_DIM)
        key_heads = rotate(raw_keys, positions).astype(jnp.bfloat16)
        value_heads = jnp.dot(normed, value_weight, preferred_element_type=jnp.float32).astype(jnp.bfloat16).reshape(LENGTH, KV_HEADS, HEAD_DIM)
        query_heads = query_rows.reshape(LENGTH, HEADS, HEAD_DIM)
        padding = jnp.zeros((margin, KV_HEADS, HEAD_DIM), jnp.bfloat16)
        padded_keys = jnp.concatenate([padding, key_heads], axis=0)
        padded_values = jnp.concatenate([padding, value_heads], axis=0)
        padded_docs = jnp.concatenate([jnp.full((margin,), -1, jnp.int32), doc_row.astype(jnp.int32)], axis=0)
        offsets = jnp.arange(block_rows, dtype=jnp.int32)
        window_offsets = jnp.arange(window, dtype=jnp.int32)

        def one_block(block_index):
            first = (block_index * block_rows).astype(jnp.int32)
            query_block = lax.dynamic_slice_in_dim(query_heads, first, block_rows, 0).astype(jnp.float32)
            query_docs = lax.dynamic_slice_in_dim(doc_row.astype(jnp.int32), first, block_rows, 0)
            query_positions = first + offsets
            key_block = lax.dynamic_slice_in_dim(padded_keys, first, window, 0)
            value_block = lax.dynamic_slice_in_dim(padded_values, first, window, 0)
            key_docs = lax.dynamic_slice_in_dim(padded_docs, first, window, 0)
            key_positions = first - margin + window_offsets
            allowed = (key_positions[None, :] <= query_positions[:, None]) & (key_docs[None, :] == query_docs[:, None])
            wide_keys = jnp.repeat(key_block, group_size, axis=1).astype(jnp.float32)
            wide_values = jnp.repeat(value_block, group_size, axis=1).astype(jnp.float32)
            scores = jnp.einsum('qnd,knd->nqk', query_block, wide_keys) * factor
            scores = jnp.where(allowed[None], scores, MASKED)
            highest = lax.optimization_barrier(jnp.max(scores, axis=-1, keepdims=True))
            exponent = jnp.where(allowed[None], jnp.exp(scores - highest), 0.0)
            weights = (exponent / lax.optimization_barrier(jnp.sum(exponent, axis=-1, keepdims=True))).astype(jnp.bfloat16)
            return jnp.einsum('nqk,knd->qnd', weights.astype(jnp.float32), wide_values).astype(jnp.bfloat16)
        blocks = lax.map(one_block, jnp.arange(LENGTH // block_rows, dtype=jnp.int32))
        return blocks.reshape(LENGTH, HEADS * HEAD_DIM)
    return lax.map(one_sequence, (hidden, queries, documents))

def reference(policy_hidden, policy_queries, policy_documents, policy_gain, policy_key_weight, policy_value_weight, frozen_hidden, frozen_queries, frozen_documents, frozen_gain, frozen_key_weight, frozen_value_weight):
    policy_mixed = one_model(policy_hidden, policy_queries, policy_documents, policy_gain, policy_key_weight, policy_value_weight)
    frozen_mixed = one_model(frozen_hidden, frozen_queries, frozen_documents, frozen_gain, frozen_key_weight, frozen_value_weight)
    return (policy_mixed, frozen_mixed)
```

```python
import functools

import jax
import jax.numpy as jnp
from jax import lax
from jax.experimental import pallas as pl
from jax.experimental.pallas import tpu as pltpu
from jax.sharding import PartitionSpec as P

HEAD_DIM = 128


EPS = 1e-05
ROPE_BASE = 500000.0
MASKED = -1e30
LANES = 128
GAIN_ROWS = 16


def rotate(raw_keys, positions):
    half_dim = HEAD_DIM // 2
    frequency = jnp.exp(
        -jnp.log(ROPE_BASE) * jnp.arange(half_dim, dtype=jnp.float32) * 2.0 / HEAD_DIM
    )
    angles = positions.astype(jnp.float32)[:, None] * frequency[None, :]
    cosines = jnp.cos(angles)[:, None, :]
    sines = jnp.sin(angles)[:, None, :]
    front_half = raw_keys[..., :half_dim]
    back_half = raw_keys[..., half_dim:]
    return jnp.concatenate(
        [front_half * cosines - back_half * sines, back_half * cosines + front_half * sines],
        axis=-1,
    )


def project(hidden, gain, key_weight, value_weight):
    tokens = hidden.shape[1]
    widened = hidden[0].astype(jnp.float32)
    inverse = lax.rsqrt(jnp.mean(widened * widened, axis=-1, keepdims=True) + EPS)
    scaled = widened * inverse
    gain_rows = lax.all_gather(gain, ("sp", "fsdp"), axis=0, tiled=True)
    key_rows = lax.all_gather(key_weight, ("sp", "fsdp"), axis=0, tiled=True)
    value_rows = lax.all_gather(value_weight, ("sp", "fsdp"), axis=0, tiled=True)
    normed = (scaled * gain_rows.astype(jnp.float32)[None, :]).astype(jnp.bfloat16)
    raw_keys = jnp.dot(normed, key_rows, preferred_element_type=jnp.float32)
    raw_values = jnp.dot(normed, value_rows, preferred_element_type=jnp.float32)
    positions = lax.axis_index("sp") * tokens + jnp.arange(tokens, dtype=jnp.int32)
    key_heads = rotate(raw_keys.reshape(tokens, -1, HEAD_DIM), positions).astype(jnp.bfloat16)
    value_heads = raw_values.astype(jnp.bfloat16).reshape(tokens, -1, HEAD_DIM)
    return (key_heads, value_heads)


def attend(queries, key_heads, value_heads, documents):
    length = queries.shape[0]
    head_count = queries.shape[1]
    block_rows = min(512, length)
    margin = min(512, length // 2)
    window = block_rows + margin
    factor = HEAD_DIM ** (-0.5)
    offsets = jnp.arange(block_rows, dtype=jnp.int32)
    window_offsets = jnp.arange(window, dtype=jnp.int32)
    padding = jnp.zeros((margin, head_count, HEAD_DIM), jnp.bfloat16)
    padded_keys = jnp.concatenate([padding, key_heads], axis=0)
    padded_values = jnp.concatenate([padding, value_heads], axis=0)
    padded_docs = jnp.concatenate([jnp.full((margin,), -1, jnp.int32), documents], axis=0)

    def one_block(block_index):
        first = block_index * block_rows
        query_block = lax.dynamic_slice_in_dim(queries, first, block_rows, 0)
        query_docs = lax.dynamic_slice_in_dim(documents, first, block_rows, 0)
        query_positions = first + offsets
        key_block = lax.dynamic_slice_in_dim(padded_keys, first, window, 0)
        value_block = lax.dynamic_slice_in_dim(padded_values, first, window, 0)
        key_docs = lax.dynamic_slice_in_dim(padded_docs, first, window, 0)
        key_positions = first - margin + window_offsets
        allowed = (key_positions[None, :] <= query_positions[:, None]) & (
            key_docs[None, :] == query_docs[:, None]
        )
        scores = (
            jnp.einsum("qnd,knd->nqk", query_block, key_block, preferred_element_type=jnp.float32)
            * factor
        )
        scores = jnp.where(allowed[None], scores, MASKED)
        highest = jnp.max(scores, axis=-1, keepdims=True)
        exponent = jnp.where(allowed[None], jnp.exp(scores - highest), 0.0)
        weights = (exponent / jnp.sum(exponent, axis=-1, keepdims=True)).astype(jnp.bfloat16)
        blended = jnp.einsum(
            "nqk,knd->qnd", weights, value_block, preferred_element_type=jnp.float32
        )
        return blended.astype(jnp.bfloat16)

    blocks = lax.map(one_block, jnp.arange(length // block_rows, dtype=jnp.int32))
    return blocks.reshape(length, head_count, HEAD_DIM)


def run_model(hidden, queries, documents, gain, key_weight, value_weight):
    tokens = hidden.shape[1]
    head_count = queries.shape[2] // HEAD_DIM
    query_local = queries[0].reshape(tokens, head_count, HEAD_DIM)
    every_doc = lax.all_gather(documents[0], "sp", axis=0, tiled=True)
    key_heads, value_heads = project(hidden, gain, key_weight, value_weight)
    group_size = head_count // key_heads.shape[1]
    wide_keys = jnp.repeat(key_heads, group_size, axis=1)
    wide_values = jnp.repeat(value_heads, group_size, axis=1)
    query_spread, key_spread, value_spread = (
        lax.all_to_all(query_local, "sp", split_axis=1, concat_axis=0, tiled=True),
        lax.all_to_all(wide_keys, "sp", split_axis=1, concat_axis=0, tiled=True),
        lax.all_to_all(wide_values, "sp", split_axis=1, concat_axis=0, tiled=True),
    )
    mixed = attend(query_spread, key_spread, value_spread, every_doc)
    returned = lax.all_to_all(mixed, "sp", split_axis=0, concat_axis=1, tiled=True)
    return returned.reshape(1, tokens, head_count * HEAD_DIM)


def gathered_weights(policy, frozen):
    return (run_model(*policy), run_model(*frozen))


def pack_kernel(hidden_p, hidden_f, queries_p, queries_f, docs_p, docs_f, out):
    planes, _, tokens, _ = out.shape
    features = hidden_p.shape[1] // planes
    per_head = queries_p.shape[1] // planes
    lane = lax.broadcasted_iota(jnp.int32, (tokens, LANES), 1)
    diagonal = lax.broadcasted_iota(jnp.int32, (tokens, tokens), 0) == lax.broadcasted_iota(
        jnp.int32, (tokens, tokens), 1
    )
    for model, (hidden, queries, docs) in enumerate(
        ((hidden_p, queries_p, docs_p), (hidden_f, queries_f, docs_f))
    ):
        widened = hidden[...].astype(jnp.float32)
        mean = jnp.sum(widened * widened, axis=-1, keepdims=True) * (1.0 / hidden.shape[1])
        inverse = lax.rsqrt(mean + EPS)
        high = inverse.astype(jnp.bfloat16).astype(jnp.float32)
        middle = (inverse - high).astype(jnp.bfloat16).astype(jnp.float32)
        low = inverse - high - middle
        doc = jnp.sum(
            jnp.where(diagonal, docs[...].astype(jnp.float32), 0.0), axis=-1, keepdims=True
        )
        side = jnp.where(lane == 0, high, 0.0)
        side = jnp.where(lane == 1, middle, side)
        side = jnp.where(lane == 2, low, side)
        side = jnp.where(lane == 3, doc, side).astype(jnp.bfloat16)
        for plane in range(planes):
            out[plane, model, :, :features] = hidden[:, plane * features : (plane + 1) * features]
            out[plane, model, :, features : features + per_head] = queries[
                :, plane * per_head : (plane + 1) * per_head
            ]
            out[plane, model, :, features + per_head :] = side


def weights_kernel(model_ref, gain_p, key_p, value_p, gain_f, key_f, value_f, keep, send):
    rows, width = key_p.shape

    def fill(out, gain, key, value):
        out[:rows, :width] = key[...]
        out[:rows, width:] = value[...]
        out[rows:, :rows] = jnp.broadcast_to(gain[...], (GAIN_ROWS, rows))

    @pl.when(model_ref[0] == 0)
    def _():
        fill(keep, gain_p, key_p, value_p)
        fill(send, gain_f, key_f, value_f)

    @pl.when(model_ref[0] != 0)
    def _():
        fill(keep, gain_f, key_f, value_f)
        fill(send, gain_p, key_p, value_p)


def partial_kernel(place_ref, packed, own_keep, own_got, pair_keep, pair_got, *outs_and_scratch):
    outs, keys, values = outs_and_scratch[:-2], outs_and_scratch[-2], outs_and_scratch[-1]
    plane, model, core = place_ref[0], place_ref[1], place_ref[2]
    planes = len(outs)
    senders, tokens, _ = packed.shape
    length = senders * tokens
    rows = own_keep.shape[0] - GAIN_ROWS
    width = own_keep.shape[1] // 2
    features = 4 * rows
    side = packed[:, :, packed.shape[2] - LANES :].reshape(length, LANES).astype(jnp.float32)
    inverse = side[:, 0:1] + side[:, 1:2] + side[:, 2:3]
    key_sum = value_sum = None
    for flip_core, flip_model, block in (
        (0, 0, own_keep),
        (0, 1, own_got),
        (1, 0, pair_keep),
        (1, 1, pair_got),
    ):
        first = pl.multiple_of(((model ^ flip_model) * 2 + (core ^ flip_core)) * rows, rows)
        hidden = packed[:, :, pl.ds(first, rows)].reshape(length, rows).astype(jnp.float32)
        gain = block[rows : rows + 1, :rows].astype(jnp.float32)
        normed = (hidden * inverse * gain).astype(jnp.bfloat16)
        key_part = jnp.dot(normed, block[:rows, :width], preferred_element_type=jnp.float32)
        value_part = jnp.dot(normed, block[:rows, width:], preferred_element_type=jnp.float32)
        key_sum = key_part if key_sum is None else key_sum + key_part
        value_sum = value_part if value_sum is None else value_sum + value_part
    for head in range(planes):
        keys[head] = key_sum[:, head * HEAD_DIM : (head + 1) * HEAD_DIM]
        values[head] = value_sum[:, head * HEAD_DIM : (head + 1) * HEAD_DIM]
    for flip in range(planes):
        outs[flip][:, :HEAD_DIM] = keys[plane ^ flip]
        outs[flip][:, HEAD_DIM:] = values[plane ^ flip]


def attend_kernel(packed, cosines, sines, *parts_and_out):
    parts, out = parts_and_out[:-1], parts_and_out[-1]
    senders, tokens, wide = packed.shape
    length = senders * tokens
    per_head = out.shape[2]
    total = parts[0][...]
    for part in parts[1:]:
        total = total + part[...]
    raw_keys = total[:, :HEAD_DIM]
    turned = jnp.concatenate(
        [raw_keys[:, HEAD_DIM // 2 :], raw_keys[:, : HEAD_DIM // 2]], axis=-1
    )
    keys = (raw_keys * cosines[...] + turned * sines[...]).astype(jnp.bfloat16)
    values = total[:, HEAD_DIM:].astype(jnp.bfloat16)
    side = packed[:, :, wide - LANES :].reshape(length, LANES).astype(jnp.float32)
    query_docs = side[:, 3:4]
    key_docs = jnp.transpose(side)[3:4, :]
    row = lax.broadcasted_iota(jnp.int32, (length, length), 0)
    column = lax.broadcasted_iota(jnp.int32, (length, length), 1)
    allowed = (column <= row) & (query_docs == key_docs)
    for head in range(per_head // HEAD_DIM):
        first = wide - LANES - per_head + head * HEAD_DIM
        queries = packed[:, :, first : first + HEAD_DIM].reshape(length, HEAD_DIM)
        scores = lax.dot_general(
            queries, keys, (((1,), (1,)), ((), ())), preferred_element_type=jnp.float32
        ) * (HEAD_DIM ** (-0.5))
        scores = jnp.where(allowed, scores, MASKED)
        highest = jnp.max(scores, axis=-1, keepdims=True)
        exponent = jnp.where(allowed, jnp.exp(scores - highest), 0.0)
        weights = (exponent / jnp.sum(exponent, axis=-1, keepdims=True)).astype(jnp.bfloat16)
        mixed = jnp.dot(weights, values, preferred_element_type=jnp.float32)
        out[:, :, head * HEAD_DIM : (head + 1) * HEAD_DIM] = mixed.astype(jnp.bfloat16).reshape(
            senders, tokens, HEAD_DIM
        )


def rotary_tables(length):
    half_dim = HEAD_DIM // 2
    frequency = jnp.exp(
        -jnp.log(ROPE_BASE) * jnp.arange(half_dim, dtype=jnp.float32) * 2.0 / HEAD_DIM
    )
    angles = jnp.arange(length, dtype=jnp.int32).astype(jnp.float32)[:, None] * frequency[None, :]
    cosines, sines = jnp.cos(angles), jnp.sin(angles)
    return (
        jnp.concatenate([cosines, cosines], axis=-1),
        jnp.concatenate([-sines, sines], axis=-1),
    )


def planes_contract(planes, policy, frozen):
    hidden_p, queries_p, docs_p, gain_p, key_p, value_p = policy
    hidden_f, queries_f, docs_f, gain_f, key_f, value_f = frozen
    tokens, depth = hidden_p.shape[1:]
    rows, width = key_p.shape
    per_head = queries_p.shape[2] // planes
    wide = depth // planes + per_head + LANES
    senders = 2 * planes
    length = senders * tokens
    place = lax.axis_index("sp")
    core = lax.axis_index("fsdp")
    plane, model = place // 2, place % 2
    vmem = pl.BlockSpec(memory_space=pltpu.VMEM)
    smem = pl.BlockSpec(memory_space=pltpu.SMEM)

    across = [(i, i ^ 1) for i in range(senders)]
    swap = [(0, 1), (1, 0)]
    keep, send = pl.pallas_call(
        weights_kernel,
        out_shape=[jax.ShapeDtypeStruct((rows + GAIN_ROWS, 2 * width), jnp.bfloat16)] * 2,
        in_specs=[smem] + [vmem] * 6,
        out_specs=[vmem] * 2,
        name="weights",
    )(
        model.reshape(1),
        gain_p.reshape(1, rows),
        key_p,
        value_p,
        gain_f.reshape(1, rows),
        key_f,
        value_f,
    )
    got = lax.ppermute(send, "sp", across)
    packed = pl.pallas_call(
        pack_kernel,
        out_shape=jax.ShapeDtypeStruct((planes, 2, tokens, wide), jnp.bfloat16),
        in_specs=[vmem] * 6,
        out_specs=vmem,
        name="pack",
    )(hidden_p[0], hidden_f[0], queries_p[0], queries_f[0], docs_p, docs_f)
    packed = lax.all_to_all(
        packed.reshape(senders, tokens, wide), "sp", split_axis=0, concat_axis=0, tiled=True
    )
    pair_keep = lax.ppermute(keep, "fsdp", swap)
    pair_got = lax.ppermute(got, "fsdp", swap)
    part_shape = jax.ShapeDtypeStruct((length, 2 * HEAD_DIM), jnp.float32)
    parts = pl.pallas_call(
        partial_kernel,
        out_shape=[part_shape] * planes,
        in_specs=[smem] + [vmem] * 5,
        out_specs=[vmem] * planes,
        scratch_shapes=[pltpu.VMEM((planes, length, HEAD_DIM), jnp.float32)] * 2,
        name="partial",
    )(jnp.stack([plane, model, core]), packed, keep, got, pair_keep, pair_got)
    arrived = [parts[0]] + [
        lax.ppermute(parts[flip], "sp", [(i, i ^ (2 * flip)) for i in range(senders)])
        for flip in range(1, planes)
    ]
    cosines, sines = rotary_tables(length)
    mixed = pl.pallas_call(
        attend_kernel,
        out_shape=jax.ShapeDtypeStruct((senders, tokens, per_head), jnp.bfloat16),
        in_specs=[vmem] * (3 + planes),
        out_specs=vmem,
        name="attend",
    )(packed, cosines, sines, *arrived)
    mixed = lax.all_to_all(mixed, "sp", split_axis=0, concat_axis=0, tiled=True)
    mixed = mixed.reshape(planes, 2, tokens, per_head).transpose(1, 2, 0, 3)
    mixed = mixed.reshape(2, 1, tokens, planes * per_head)
    return (mixed[0], mixed[1])


def per_device(sp_size, fsdp_size, *arrays):
    policy, frozen = arrays[:6], arrays[6:]
    key_heads = policy[4].shape[1] // HEAD_DIM
    tokens, depth = policy[0].shape[1:]
    planes = sp_size // 2
    if (
        sp_size == 2 * key_heads
        and planes & (planes - 1) == 0
        and fsdp_size == 2
        and tokens % 16 == 0
        and policy[4].shape[0] % LANES == 0
        and 2 * policy[4].shape[0] <= 2 * policy[4].shape[1]
        and sp_size * tokens <= 512
    ):
        return planes_contract(planes, policy, frozen)
    return gathered_weights(policy, frozen)


def solution(mesh):
    return jax.shard_map(
        functools.partial(per_device, mesh.shape["sp"], mesh.shape["fsdp"]),
        mesh=mesh,
        in_specs=(
            P(("groups", "fsdp"), "sp", None),
            P(("groups", "fsdp"), "sp", None),
            P(("groups", "fsdp"), "sp"),
            P(("sp", "fsdp")),
            P(("sp", "fsdp"), None),
            P(("sp", "fsdp"), None),
            P(("groups", "fsdp"), "sp", None),
            P(("groups", "fsdp"), "sp", None),
            P(("groups", "fsdp"), "sp"),
            P(("sp", "fsdp")),
            P(("sp", "fsdp"), None),
            P(("sp", "fsdp"), None),
        ),
        out_specs=(P(("groups", "fsdp"), "sp", None), P(("groups", "fsdp"), "sp", None)),
        check_vma=False,
    )
```

```python
import functools

import jax
import jax.numpy as jnp
from jax import lax
from jax.experimental import pallas as pl
from jax.experimental.pallas import tpu as pltpu
from jax.sharding import PartitionSpec as P


HEAD_DIM = 128


EPS = 1e-05
ROPE_BASE = 500000.0
MASKED = -1e30
LANES = 128
GAIN_ROWS = 16
KERNEL_BYTES = 16 * 2**20


def rotate(raw_keys, positions):
    half_dim = HEAD_DIM // 2
    frequency = jnp.exp(
        -jnp.log(ROPE_BASE) * jnp.arange(half_dim, dtype=jnp.float32) * 2.0 / HEAD_DIM
    )
    angles = positions.astype(jnp.float32)[:, None] * frequency[None, :]
    cosines = jnp.cos(angles)[:, None, :]
    sines = jnp.sin(angles)[:, None, :]
    front_half = raw_keys[..., :half_dim]
    back_half = raw_keys[..., half_dim:]
    return jnp.concatenate(
        [front_half * cosines - back_half * sines, back_half * cosines + front_half * sines],
        axis=-1,
    )


def project(hidden, gain, key_weight, value_weight):
    tokens = hidden.shape[1]
    widened = hidden[0].astype(jnp.float32)
    inverse = lax.rsqrt(jnp.mean(widened * widened, axis=-1, keepdims=True) + EPS)
    scaled = widened * inverse
    gain_rows = lax.all_gather(gain, ("sp", "fsdp"), axis=0, tiled=True)
    key_rows = lax.all_gather(key_weight, ("sp", "fsdp"), axis=0, tiled=True)
    value_rows = lax.all_gather(value_weight, ("sp", "fsdp"), axis=0, tiled=True)
    normed = (scaled * gain_rows.astype(jnp.float32)[None, :]).astype(jnp.bfloat16)
    raw_keys = jnp.dot(normed, key_rows, preferred_element_type=jnp.float32)
    raw_values = jnp.dot(normed, value_rows, preferred_element_type=jnp.float32)
    positions = lax.axis_index("sp") * tokens + jnp.arange(tokens, dtype=jnp.int32)
    key_heads = rotate(raw_keys.reshape(tokens, -1, HEAD_DIM), positions).astype(jnp.bfloat16)
    value_heads = raw_values.astype(jnp.bfloat16).reshape(tokens, -1, HEAD_DIM)
    return (key_heads, value_heads)


def attend(queries, key_heads, value_heads, documents):
    length = queries.shape[0]
    head_count = queries.shape[1]
    block_rows = min(512, length)
    margin = min(512, length // 2)
    window = block_rows + margin
    factor = HEAD_DIM ** (-0.5)
    offsets = jnp.arange(block_rows, dtype=jnp.int32)
    window_offsets = jnp.arange(window, dtype=jnp.int32)
    padding = jnp.zeros((margin, head_count, HEAD_DIM), jnp.bfloat16)
    padded_keys = jnp.concatenate([padding, key_heads], axis=0)
    padded_values = jnp.concatenate([padding, value_heads], axis=0)
    padded_docs = jnp.concatenate([jnp.full((margin,), -1, jnp.int32), documents], axis=0)

    def one_block(block_index):
        first = block_index * block_rows
        query_block = lax.dynamic_slice_in_dim(queries, first, block_rows, 0)
        query_docs = lax.dynamic_slice_in_dim(documents, first, block_rows, 0)
        query_positions = first + offsets
        key_block = lax.dynamic_slice_in_dim(padded_keys, first, window, 0)
        value_block = lax.dynamic_slice_in_dim(padded_values, first, window, 0)
        key_docs = lax.dynamic_slice_in_dim(padded_docs, first, window, 0)
        key_positions = first - margin + window_offsets
        allowed = (key_positions[None, :] <= query_positions[:, None]) & (
            key_docs[None, :] == query_docs[:, None]
        )
        scores = (
            jnp.einsum("qnd,knd->nqk", query_block, key_block, preferred_element_type=jnp.float32)
            * factor
        )
        scores = jnp.where(allowed[None], scores, MASKED)
        highest = jnp.max(scores, axis=-1, keepdims=True)
        exponent = jnp.where(allowed[None], jnp.exp(scores - highest), 0.0)
        weights = (exponent / jnp.sum(exponent, axis=-1, keepdims=True)).astype(jnp.bfloat16)
        blended = jnp.einsum(
            "nqk,knd->qnd", weights, value_block, preferred_element_type=jnp.float32
        )
        return blended.astype(jnp.bfloat16)

    blocks = lax.map(one_block, jnp.arange(length // block_rows, dtype=jnp.int32))
    return blocks.reshape(length, head_count, HEAD_DIM)


def run_model(hidden, queries, documents, gain, key_weight, value_weight):
    tokens = hidden.shape[1]
    head_count = queries.shape[2] // HEAD_DIM
    query_local = queries[0].reshape(tokens, head_count, HEAD_DIM)
    every_doc = lax.all_gather(documents[0], "sp", axis=0, tiled=True)
    key_heads, value_heads = project(hidden, gain, key_weight, value_weight)
    group_size = head_count // key_heads.shape[1]
    wide_keys = jnp.repeat(key_heads, group_size, axis=1)
    wide_values = jnp.repeat(value_heads, group_size, axis=1)
    query_spread, key_spread, value_spread = (
        lax.all_to_all(query_local, "sp", split_axis=1, concat_axis=0, tiled=True),
        lax.all_to_all(wide_keys, "sp", split_axis=1, concat_axis=0, tiled=True),
        lax.all_to_all(wide_values, "sp", split_axis=1, concat_axis=0, tiled=True),
    )
    mixed = attend(query_spread, key_spread, value_spread, every_doc)
    returned = lax.all_to_all(mixed, "sp", split_axis=0, concat_axis=1, tiled=True)
    return returned.reshape(1, tokens, head_count * HEAD_DIM)


def gathered_weights(policy, frozen):
    return (run_model(*policy), run_model(*frozen))


def pack_kernel(
    gain_p,
    key_p,
    value_p,
    gain_f,
    key_f,
    value_f,
    hidden_p,
    hidden_f,
    queries_p,
    queries_f,
    docs_p,
    docs_f,
    send,
    keep,
    out,
):
    rows, width = key_p.shape

    def fill(target, gain, key, value):
        target[:rows, :width] = key[...]
        target[:rows, width:] = value[...]
        target[rows:, :rows] = jnp.broadcast_to(gain[...].reshape(1, rows), (GAIN_ROWS, rows))

    model = lax.axis_index("sp") % 2

    @pl.when(model == 0)
    def _():
        fill(send, gain_f, key_f, value_f)
        fill(keep, gain_p, key_p, value_p)

    @pl.when(model != 0)
    def _():
        fill(send, gain_p, key_p, value_p)
        fill(keep, gain_f, key_f, value_f)

    planes, _, tokens, _ = out.shape
    features = hidden_p.shape[1] // planes
    per_head = queries_p.shape[1] // planes
    lane = lax.broadcasted_iota(jnp.int32, (tokens, LANES), 1)
    diagonal = lax.broadcasted_iota(jnp.int32, (tokens, tokens), 0) == lax.broadcasted_iota(
        jnp.int32, (tokens, tokens), 1
    )
    for owner, (hidden, queries, docs) in enumerate(
        ((hidden_p, queries_p, docs_p), (hidden_f, queries_f, docs_f))
    ):
        widened = hidden[...].astype(jnp.float32)
        mean = jnp.sum(widened * widened, axis=-1, keepdims=True) * (1.0 / hidden.shape[1])
        inverse = lax.rsqrt(mean + EPS)
        high = inverse.astype(jnp.bfloat16).astype(jnp.float32)
        middle = (inverse - high).astype(jnp.bfloat16).astype(jnp.float32)
        low = inverse - high - middle
        doc = jnp.sum(
            jnp.where(diagonal, docs[...].astype(jnp.float32), 0.0), axis=-1, keepdims=True
        )
        side = jnp.where(lane == 0, high, 0.0)
        side = jnp.where(lane == 1, middle, side)
        side = jnp.where(lane == 2, low, side)
        side = jnp.where(lane == 3, doc, side).astype(jnp.bfloat16)
        for plane in range(planes):
            out[plane, owner, :, :features] = hidden[:, plane * features : (plane + 1) * features]
            out[plane, owner, :, features : features + per_head] = queries[
                :, plane * per_head : (plane + 1) * per_head
            ]
            out[plane, owner, :, features + per_head :] = side


def partial_kernel(packed, own_keep, own_got, pair_keep, pair_got, *outs_and_scratch):
    outs, keys, values = outs_and_scratch[:-2], outs_and_scratch[-2], outs_and_scratch[-1]
    place, core = lax.axis_index("sp"), lax.axis_index("fsdp")
    plane, model = place // 2, place % 2
    planes = len(outs)
    senders, tokens, _ = packed.shape
    length = senders * tokens
    rows = own_keep.shape[0] - GAIN_ROWS
    width = own_keep.shape[1] // 2
    side = packed[:, :, packed.shape[2] - LANES :].reshape(length, LANES).astype(jnp.float32)
    inverse = side[:, 0:1] + side[:, 1:2] + side[:, 2:3]
    key_sum = value_sum = None
    for flip_core, flip_model, block in (
        (0, 0, own_keep),
        (0, 1, own_got),
        (1, 0, pair_keep),
        (1, 1, pair_got),
    ):
        first = pl.multiple_of(((model ^ flip_model) * 2 + (core ^ flip_core)) * rows, rows)
        hidden = packed[:, :, pl.ds(first, rows)].reshape(length, rows).astype(jnp.float32)
        gain = block[rows : rows + 1, :rows].astype(jnp.float32)
        normed = (hidden * inverse * gain).astype(jnp.bfloat16)
        key_part = jnp.dot(normed, block[:rows, :width], preferred_element_type=jnp.float32)
        value_part = jnp.dot(normed, block[:rows, width:], preferred_element_type=jnp.float32)
        key_sum = key_part if key_sum is None else key_sum + key_part
        value_sum = value_part if value_sum is None else value_sum + value_part
    for head in range(planes):
        keys[head] = key_sum[:, head * HEAD_DIM : (head + 1) * HEAD_DIM]
        values[head] = value_sum[:, head * HEAD_DIM : (head + 1) * HEAD_DIM]
    for flip in range(planes):
        outs[flip][:, :HEAD_DIM] = keys[plane ^ flip]
        outs[flip][:, HEAD_DIM:] = values[plane ^ flip]


def attend_kernel(packed, cosines, sines, *parts_and_out):
    parts, out = parts_and_out[:-1], parts_and_out[-1]
    senders, tokens, wide = packed.shape
    length = senders * tokens
    per_head = out.shape[2]
    total = parts[0][...]
    for part in parts[1:]:
        total = total + part[...]
    raw_keys = total[:, :HEAD_DIM]
    turned = jnp.concatenate(
        [raw_keys[:, HEAD_DIM // 2 :], raw_keys[:, : HEAD_DIM // 2]], axis=-1
    )
    keys = (raw_keys * cosines[...] + turned * sines[...]).astype(jnp.bfloat16)
    values = total[:, HEAD_DIM:].astype(jnp.bfloat16)
    side = packed[:, :, wide - LANES :].reshape(length, LANES).astype(jnp.float32)
    query_docs = side[:, 3:4]
    key_docs = jnp.transpose(side)[3:4, :]
    row = lax.broadcasted_iota(jnp.int32, (length, length), 0)
    column = lax.broadcasted_iota(jnp.int32, (length, length), 1)
    allowed = (column <= row) & (query_docs == key_docs)
    for head in range(per_head // HEAD_DIM):
        first = wide - LANES - per_head + head * HEAD_DIM
        queries = packed[:, :, first : first + HEAD_DIM].reshape(length, HEAD_DIM)
        scores = lax.dot_general(
            queries, keys, (((1,), (1,)), ((), ())), preferred_element_type=jnp.float32
        ) * (HEAD_DIM ** (-0.5))
        scores = jnp.where(allowed, scores, MASKED)
        highest = jnp.max(scores, axis=-1, keepdims=True)
        exponent = jnp.where(allowed, jnp.exp(scores - highest), 0.0)
        weights = (exponent / jnp.sum(exponent, axis=-1, keepdims=True)).astype(jnp.bfloat16)
        mixed = jnp.dot(weights, values, preferred_element_type=jnp.float32)
        out[:, :, head * HEAD_DIM : (head + 1) * HEAD_DIM] = mixed.astype(jnp.bfloat16).reshape(
            senders, tokens, HEAD_DIM
        )


def here(x):
    return pltpu.with_memory_space_constraint(x, pltpu.VMEM)


def there(x):
    return pltpu.with_memory_space_constraint(x, pltpu.HBM)


def rotary_tables(length):
    half_dim = HEAD_DIM // 2
    frequency = jnp.exp(
        -jnp.log(ROPE_BASE) * jnp.arange(half_dim, dtype=jnp.float32) * 2.0 / HEAD_DIM
    )
    angles = jnp.arange(length, dtype=jnp.int32).astype(jnp.float32)[:, None] * frequency[None, :]
    cosines, sines = jnp.cos(angles), jnp.sin(angles)
    return (
        jnp.concatenate([cosines, cosines], axis=-1),
        jnp.concatenate([-sines, sines], axis=-1),
    )


def planes_contract(planes, policy, frozen):
    hidden_p, queries_p, docs_p, gain_p, key_p, value_p = policy
    hidden_f, queries_f, docs_f, gain_f, key_f, value_f = frozen
    tokens, depth = hidden_p.shape[1:]
    rows, width = key_p.shape
    per_head = queries_p.shape[2] // planes
    wide = depth // planes + per_head + LANES
    senders = 2 * planes
    length = senders * tokens
    vmem = pl.BlockSpec(memory_space=pltpu.VMEM)

    across = [(i, i ^ 1) for i in range(senders)]
    swap = [(0, 1), (1, 0)]
    weights_shape = pltpu.VMEM((rows + GAIN_ROWS, 2 * width), jnp.bfloat16)
    send, keep, packed = pl.pallas_call(
        pack_kernel,
        out_shape=[
            weights_shape,
            weights_shape,
            pltpu.VMEM((planes, 2, tokens, wide), jnp.bfloat16),
        ],
        in_specs=[vmem] * 12,
        out_specs=[vmem] * 3,
        compiler_params=pltpu.CompilerParams(vmem_limit_bytes=KERNEL_BYTES),
        name="pack",
    )(
        *(
            there(array)
            for array in (
                gain_p,
                key_p,
                value_p,
                gain_f,
                key_f,
                value_f,
                hidden_p[0],
                hidden_f[0],
                queries_p[0],
                queries_f[0],
                docs_p,
                docs_f,
            )
        ),
    )
    got = lax.ppermute(send, "sp", across)
    packed = lax.all_to_all(
        packed.reshape(senders, tokens, wide), "sp", split_axis=0, concat_axis=0, tiled=True
    )
    pair_keep = lax.ppermute(keep, "fsdp", swap)
    pair_got = lax.ppermute(got, "fsdp", swap)
    part_shape = pltpu.VMEM((length, 2 * HEAD_DIM), jnp.float32)
    packed = here(packed)
    parts = pl.pallas_call(
        partial_kernel,
        out_shape=[part_shape] * planes,
        in_specs=[vmem] * 5,
        out_specs=[vmem] * planes,
        scratch_shapes=[pltpu.VMEM((planes, length, HEAD_DIM), jnp.float32)] * 2,
        compiler_params=pltpu.CompilerParams(vmem_limit_bytes=KERNEL_BYTES),
        name="partial",
    )(packed, here(keep), here(got), here(pair_keep), here(pair_got))
    arrived = [parts[0]] + [
        lax.ppermute(parts[flip], "sp", [(i, i ^ (2 * flip)) for i in range(senders)])
        for flip in reversed(range(1, planes))
    ]
    cosines, sines = rotary_tables(length)
    mixed = pl.pallas_call(
        attend_kernel,
        out_shape=pltpu.VMEM((senders, tokens, per_head), jnp.bfloat16),
        in_specs=[vmem] * (3 + planes),
        out_specs=vmem,
        compiler_params=pltpu.CompilerParams(vmem_limit_bytes=KERNEL_BYTES),
        name="attend",
    )(packed, cosines, sines, *(here(part) for part in arrived))
    mixed = lax.all_to_all(mixed, "sp", split_axis=0, concat_axis=0, tiled=True)
    mixed = mixed.reshape(planes, 2, tokens, per_head).transpose(1, 2, 0, 3)
    mixed = mixed.reshape(2, 1, tokens, planes * per_head)
    return (mixed[0], mixed[1])


def per_device(sp_size, fsdp_size, *arrays):
    policy, frozen = arrays[:6], arrays[6:]
    key_heads = policy[4].shape[1] // HEAD_DIM
    tokens, _ = policy[0].shape[1:]
    planes = sp_size // 2
    if (
        sp_size == 2 * key_heads
        and planes & (planes - 1) == 0
        and fsdp_size == 2
        and tokens % 16 == 0
        and policy[4].shape[0] % LANES == 0
        and 2 * policy[4].shape[0] <= 2 * policy[4].shape[1]
        and sp_size * tokens <= 512
    ):
        return planes_contract(planes, policy, frozen)
    return gathered_weights(policy, frozen)


def solution(mesh):
    return jax.shard_map(
        functools.partial(per_device, mesh.shape["sp"], mesh.shape["fsdp"]),
        mesh=mesh,
        in_specs=(
            P(("groups", "fsdp"), "sp", None),
            P(("groups", "fsdp"), "sp", None),
            P(("groups", "fsdp"), "sp"),
            P(("sp", "fsdp")),
            P(("sp", "fsdp"), None),
            P(("sp", "fsdp"), None),
            P(("groups", "fsdp"), "sp", None),
            P(("groups", "fsdp"), "sp", None),
            P(("groups", "fsdp"), "sp"),
            P(("sp", "fsdp")),
            P(("sp", "fsdp"), None),
            P(("sp", "fsdp"), None),
        ),
        out_specs=(P(("groups", "fsdp"), "sp", None), P(("groups", "fsdp"), "sp", None)),
        check_vma=False,
    )
```

```python
import functools

import jax
import jax.numpy as jnp
from jax import lax
from jax.experimental import pallas as pl
from jax.experimental.pallas import tpu as pltpu
from jax.sharding import PartitionSpec as P


HEAD_DIM = 128


EPS = 1e-05
ROPE_BASE = 500000.0
MASKED = -1e30
LANES = 128
SIDE_ROWS = 8
SIDE_GAINS = 4
KERNEL_BYTES = 16 * 2**20


def rotate(raw_keys, positions):
    half_dim = HEAD_DIM // 2
    frequency = jnp.exp(
        -jnp.log(ROPE_BASE) * jnp.arange(half_dim, dtype=jnp.float32) * 2.0 / HEAD_DIM
    )
    angles = positions.astype(jnp.float32)[:, None] * frequency[None, :]
    cosines = jnp.cos(angles)[:, None, :]
    sines = jnp.sin(angles)[:, None, :]
    front_half = raw_keys[..., :half_dim]
    back_half = raw_keys[..., half_dim:]
    return jnp.concatenate(
        [front_half * cosines - back_half * sines, back_half * cosines + front_half * sines],
        axis=-1,
    )


def project(hidden, gain, key_weight, value_weight):
    tokens = hidden.shape[1]
    widened = hidden[0].astype(jnp.float32)
    inverse = lax.rsqrt(jnp.mean(widened * widened, axis=-1, keepdims=True) + EPS)
    scaled = widened * inverse
    gain_rows = lax.all_gather(gain, ("sp", "fsdp"), axis=0, tiled=True)
    key_rows = lax.all_gather(key_weight, ("sp", "fsdp"), axis=0, tiled=True)
    value_rows = lax.all_gather(value_weight, ("sp", "fsdp"), axis=0, tiled=True)
    normed = (scaled * gain_rows.astype(jnp.float32)[None, :]).astype(jnp.bfloat16)
    raw_keys = jnp.dot(normed, key_rows, preferred_element_type=jnp.float32)
    raw_values = jnp.dot(normed, value_rows, preferred_element_type=jnp.float32)
    positions = lax.axis_index("sp") * tokens + jnp.arange(tokens, dtype=jnp.int32)
    key_heads = rotate(raw_keys.reshape(tokens, -1, HEAD_DIM), positions).astype(jnp.bfloat16)
    value_heads = raw_values.astype(jnp.bfloat16).reshape(tokens, -1, HEAD_DIM)
    return (key_heads, value_heads)


def attend(queries, key_heads, value_heads, documents):
    length = queries.shape[0]
    head_count = queries.shape[1]
    block_rows = min(512, length)
    margin = min(512, length // 2)
    window = block_rows + margin
    factor = HEAD_DIM ** (-0.5)
    offsets = jnp.arange(block_rows, dtype=jnp.int32)
    window_offsets = jnp.arange(window, dtype=jnp.int32)
    padding = jnp.zeros((margin, head_count, HEAD_DIM), jnp.bfloat16)
    padded_keys = jnp.concatenate([padding, key_heads], axis=0)
    padded_values = jnp.concatenate([padding, value_heads], axis=0)
    padded_docs = jnp.concatenate([jnp.full((margin,), -1, jnp.int32), documents], axis=0)

    def one_block(block_index):
        first = block_index * block_rows
        query_block = lax.dynamic_slice_in_dim(queries, first, block_rows, 0)
        query_docs = lax.dynamic_slice_in_dim(documents, first, block_rows, 0)
        query_positions = first + offsets
        key_block = lax.dynamic_slice_in_dim(padded_keys, first, window, 0)
        value_block = lax.dynamic_slice_in_dim(padded_values, first, window, 0)
        key_docs = lax.dynamic_slice_in_dim(padded_docs, first, window, 0)
        key_positions = first - margin + window_offsets
        allowed = (key_positions[None, :] <= query_positions[:, None]) & (
            key_docs[None, :] == query_docs[:, None]
        )
        scores = (
            jnp.einsum("qnd,knd->nqk", query_block, key_block, preferred_element_type=jnp.float32)
            * factor
        )
        scores = jnp.where(allowed[None], scores, MASKED)
        highest = jnp.max(scores, axis=-1, keepdims=True)
        exponent = jnp.where(allowed[None], jnp.exp(scores - highest), 0.0)
        weights = (exponent / jnp.sum(exponent, axis=-1, keepdims=True)).astype(jnp.bfloat16)
        blended = jnp.einsum(
            "nqk,knd->qnd", weights, value_block, preferred_element_type=jnp.float32
        )
        return blended.astype(jnp.bfloat16)

    blocks = lax.map(one_block, jnp.arange(length // block_rows, dtype=jnp.int32))
    return blocks.reshape(length, head_count, HEAD_DIM)


def run_model(hidden, queries, documents, gain, key_weight, value_weight):
    tokens = hidden.shape[1]
    head_count = queries.shape[2] // HEAD_DIM
    query_local = queries[0].reshape(tokens, head_count, HEAD_DIM)
    every_doc = lax.all_gather(documents[0], "sp", axis=0, tiled=True)
    key_heads, value_heads = project(hidden, gain, key_weight, value_weight)
    group_size = head_count // key_heads.shape[1]
    wide_keys = jnp.repeat(key_heads, group_size, axis=1)
    wide_values = jnp.repeat(value_heads, group_size, axis=1)
    query_spread, key_spread, value_spread = (
        lax.all_to_all(query_local, "sp", split_axis=1, concat_axis=0, tiled=True),
        lax.all_to_all(wide_keys, "sp", split_axis=1, concat_axis=0, tiled=True),
        lax.all_to_all(wide_values, "sp", split_axis=1, concat_axis=0, tiled=True),
    )
    mixed = attend(query_spread, key_spread, value_spread, every_doc)
    returned = lax.all_to_all(mixed, "sp", split_axis=0, concat_axis=1, tiled=True)
    return returned.reshape(1, tokens, head_count * HEAD_DIM)


def gathered_weights(policy, frozen):
    return (run_model(*policy), run_model(*frozen))


def weights_kernel(key_p, value_p, key_f, value_f, send, keep, sems):
    _, width = key_p.shape
    half = send.shape[0]
    model = lax.axis_index("sp") // (lax.axis_size("sp") // 2)
    first = pl.multiple_of(lax.axis_index("groups") * half, half)

    def move(key_own, value_own, key_other, value_other):
        copies = [
            pltpu.make_async_copy(source, target, sems.at[index])
            for index, (source, target) in enumerate(
                (
                    (key_other.at[pl.ds(first, half), :], send.at[:, :width]),
                    (value_other.at[pl.ds(first, half), :], send.at[:, width:]),
                    (key_own, keep.at[:, :width]),
                    (value_own, keep.at[:, width:]),
                )
            )
        ]
        for copy in copies:
            copy.start()
        for copy in copies:
            copy.wait()

    @pl.when(model == 0)
    def _():
        move(key_p, value_p, key_f, value_f)

    @pl.when(model != 0)
    def _():
        move(key_f, value_f, key_p, value_p)


def pack_kernel(
    gain_p,
    gain_f,
    pair_gain_p,
    pair_gain_f,
    hidden_p,
    hidden_f,
    queries_p,
    queries_f,
    docs_p,
    docs_f,
    out,
):
    _, units, _, _ = out.shape
    tokens, depth = hidden_p.shape
    rows = gain_p.shape[0]
    block = 2 * rows
    tiles = block // LANES
    per_head = queries_p.shape[1] // units
    row = lax.broadcasted_iota(jnp.int32, (SIDE_ROWS, LANES), 0)
    diagonal = lax.broadcasted_iota(jnp.int32, (tokens, LANES), 0) == lax.broadcasted_iota(
        jnp.int32, (tokens, LANES), 1
    )

    def turned(column):
        return jnp.sum(jnp.where(diagonal, column, 0.0), axis=0, keepdims=True)

    for owner, (hidden, queries, docs, gain, pair_gain) in enumerate(
        (
            (hidden_p, queries_p, docs_p, gain_p, pair_gain_p),
            (hidden_f, queries_f, docs_f, gain_f, pair_gain_f),
        )
    ):
        widened = hidden[...].astype(jnp.float32)
        mean = jnp.sum(widened * widened, axis=-1, keepdims=True) * (1.0 / depth)
        inverse = lax.rsqrt(mean + EPS)
        high = inverse.astype(jnp.bfloat16).astype(jnp.float32)
        middle = (inverse - high).astype(jnp.bfloat16).astype(jnp.float32)
        low = inverse - high - middle
        doc = jnp.concatenate(
            [docs[...].astype(jnp.float32), jnp.zeros((1, LANES - tokens), jnp.float32)], axis=-1
        )
        gains = [gain[...].reshape(1, rows).astype(jnp.float32)]
        gains.append(pair_gain[...].reshape(1, rows).astype(jnp.float32))
        side = jnp.where(row == 0, turned(high), 0.0)
        side = jnp.where(row == 1, turned(middle), side)
        side = jnp.where(row == 2, turned(low), side)
        side = jnp.where(row == 3, doc, side)
        for which in range(2):
            for part in range(rows // LANES):
                side = jnp.where(
                    row == SIDE_GAINS + which * (rows // LANES) + part,
                    gains[which][:, part * LANES : (part + 1) * LANES],
                    side,
                )
        side = side.astype(jnp.bfloat16)
        for unit in range(units):
            for tile in range(2 * tiles):
                first = (unit + (tile // tiles) * units) * block + (tile % tiles) * LANES
                out[owner, unit, tile * tokens : (tile + 1) * tokens, :] = hidden[
                    :, first : first + LANES
                ]
            for tile in range(per_head // LANES):
                first = unit * per_head + tile * LANES
                low = (2 * tiles + tile) * tokens
                out[owner, unit, low : low + tokens, :] = queries[:, first : first + LANES]
            out[owner, unit, out.shape[2] - SIDE_ROWS :, :] = side


def side_columns(packed, tokens, sums):
    senders, high, _ = packed.shape
    side = packed[:, high - SIDE_ROWS :, :].reshape(senders * SIDE_ROWS, LANES)
    turned = jnp.transpose(side.astype(jnp.float32))
    columns = []
    for sender in range(senders):
        column = None
        for index in sums:
            first = sender * SIDE_ROWS + index
            part = turned[:tokens, first : first + 1]
            column = part if column is None else column + part
        columns.append(column)
    return jnp.concatenate(columns, axis=0)


def partial_kernel(
    tokens, packed, keep, got, far, pair_keep, pair_got, pair_far, *outs_and_scratch
):
    outs, keys, values = outs_and_scratch[:-2], outs_and_scratch[-2], outs_and_scratch[-1]
    units = len(outs)
    place, core, group = lax.axis_index("sp"), lax.axis_index("fsdp"), lax.axis_index("groups")
    model, unit = place // units, place % units
    senders, high, _ = packed.shape
    length = senders * tokens
    half = got.shape[0]
    width = keep.shape[1] // 2
    halves = keep.shape[0] // half
    strips = half // LANES
    inverse = side_columns(packed, tokens, (0, 1, 2))
    first_side = high - SIDE_ROWS
    key_sum = value_sum = None
    for weights, flip_model, flip_core, part in (
        (keep, 0, 0, 0),
        (keep, 0, 0, 1),
        (got, 1, 0, group),
        (far, 1, 0, 1 - group),
        (pair_keep, 0, 1, 0),
        (pair_keep, 0, 1, 1),
        (pair_got, 1, 1, group),
        (pair_far, 1, 1, 1 - group),
    ):
        source = model ^ flip_model
        side = packed[source * units + unit, first_side:, :].astype(jnp.float32)
        columns = []
        for strip in range(strips):
            tile = ((source * 2 + (core ^ flip_core)) * halves + part) * strips + strip
            hidden = packed[:, pl.ds(pl.multiple_of(tile * tokens, tokens), tokens), :]
            hidden = hidden.reshape(length, LANES).astype(jnp.float32)
            wanted = SIDE_GAINS + (flip_core * halves + part) * strips + strip
            picked = lax.broadcasted_iota(jnp.int32, (SIDE_ROWS, LANES), 0) == wanted
            gain = jnp.sum(jnp.where(picked, side, 0.0), axis=0, keepdims=True)
            columns.append((hidden * inverse * gain).astype(jnp.bfloat16))
        normed = jnp.concatenate(columns, axis=-1) if strips > 1 else columns[0]
        low = part * half if weights is keep or weights is pair_keep else 0
        key_part = jnp.dot(
            normed, weights[low : low + half, :width], preferred_element_type=jnp.float32
        )
        value_part = jnp.dot(
            normed, weights[low : low + half, width:], preferred_element_type=jnp.float32
        )
        key_sum = key_part if key_sum is None else key_sum + key_part
        value_sum = value_part if value_sum is None else value_sum + value_part
    for head in range(units):
        keys[head] = key_sum[:, head * HEAD_DIM : (head + 1) * HEAD_DIM]
        values[head] = value_sum[:, head * HEAD_DIM : (head + 1) * HEAD_DIM]
    for flip in range(units):
        outs[flip][:, :HEAD_DIM] = keys[unit ^ flip]
        outs[flip][:, HEAD_DIM:] = values[unit ^ flip]


def attend_kernel(tokens, packed, cosines, sines, *parts_and_out):
    parts, out = parts_and_out[:-1], parts_and_out[-1]
    senders = packed.shape[0]
    length = senders * tokens
    per_head = out.shape[2]
    total = parts[0][...]
    for part in parts[1:]:
        total = total + part[...]
    raw_keys = total[:, :HEAD_DIM]
    turned = jnp.concatenate(
        [raw_keys[:, HEAD_DIM // 2 :], raw_keys[:, : HEAD_DIM // 2]], axis=-1
    )
    keys = (raw_keys * cosines[...] + turned * sines[...]).astype(jnp.bfloat16)
    values = total[:, HEAD_DIM:].astype(jnp.bfloat16)
    query_docs = side_columns(packed, tokens, (3,))
    key_docs = jnp.transpose(jnp.broadcast_to(query_docs, (length, LANES)))[:1, :]
    row = lax.broadcasted_iota(jnp.int32, (length, length), 0)
    column = lax.broadcasted_iota(jnp.int32, (length, length), 1)
    allowed = (column <= row) & (query_docs == key_docs)
    for head in range(per_head // HEAD_DIM):
        low = packed.shape[1] - SIDE_ROWS - (per_head // HEAD_DIM - head) * tokens
        queries = packed[:, low : low + tokens, :].reshape(length, HEAD_DIM)
        scores = lax.dot_general(
            queries, keys, (((1,), (1,)), ((), ())), preferred_element_type=jnp.float32
        ) * (HEAD_DIM ** (-0.5))
        scores = jnp.where(allowed, scores, MASKED)
        highest = jnp.max(scores, axis=-1, keepdims=True)
        exponent = jnp.where(allowed, jnp.exp(scores - highest), 0.0)
        weights = (exponent / jnp.sum(exponent, axis=-1, keepdims=True)).astype(jnp.bfloat16)
        mixed = jnp.dot(weights, values, preferred_element_type=jnp.float32)
        out[:, :, head * HEAD_DIM : (head + 1) * HEAD_DIM] = mixed.astype(jnp.bfloat16).reshape(
            senders, tokens, HEAD_DIM
        )


def here(x):
    return pltpu.with_memory_space_constraint(x, pltpu.VMEM)


def assemble_kernel(arrived, out_p, out_f):
    _, units, _, per_head = arrived.shape
    for owner, out in enumerate((out_p, out_f)):
        for unit in range(units):
            out[:, unit * per_head : (unit + 1) * per_head] = arrived[owner, unit]


def there(x):
    return pltpu.with_memory_space_constraint(x, pltpu.HBM)


def rotary_tables(length):
    half_dim = HEAD_DIM // 2
    frequency = jnp.exp(
        -jnp.log(ROPE_BASE) * jnp.arange(half_dim, dtype=jnp.float32) * 2.0 / HEAD_DIM
    )
    angles = jnp.arange(length, dtype=jnp.int32).astype(jnp.float32)[:, None] * frequency[None, :]
    cosines, sines = jnp.cos(angles), jnp.sin(angles)
    return (
        jnp.concatenate([cosines, cosines], axis=-1),
        jnp.concatenate([-sines, sines], axis=-1),
    )


def halves_contract(units, policy, frozen):
    hidden_p, queries_p, docs_p, gain_p, key_p, value_p = policy
    hidden_f, queries_f, docs_f, gain_f, key_f, value_f = frozen
    tokens = hidden_p.shape[1]
    rows, width = key_p.shape
    half = rows // 2
    per_head = queries_p.shape[2] // units
    senders = 2 * units
    length = senders * tokens
    high = (4 * rows + per_head) // LANES * tokens + SIDE_ROWS
    vmem = pl.BlockSpec(memory_space=pltpu.VMEM)
    hbm = pl.BlockSpec(memory_space=pltpu.HBM)
    params = pltpu.CompilerParams(vmem_limit_bytes=KERNEL_BYTES)
    swap = [(0, 1), (1, 0)]

    send, keep = pl.pallas_call(
        weights_kernel,
        out_shape=[
            pltpu.VMEM((half, 2 * width), jnp.bfloat16),
            pltpu.VMEM((rows, 2 * width), jnp.bfloat16),
        ],
        in_specs=[hbm] * 4,
        out_specs=[vmem] * 2,
        scratch_shapes=[pltpu.SemaphoreType.DMA((4,))],
        compiler_params=params,
        name="weights",
    )(*(there(array) for array in (key_p, value_p, key_f, value_f)))
    got = lax.ppermute(send, "sp", [(i, i ^ units) for i in range(senders)])
    pair_gain_p = lax.ppermute(gain_p, "fsdp", swap)
    pair_gain_f = lax.ppermute(gain_f, "fsdp", swap)
    packed = pl.pallas_call(
        pack_kernel,
        out_shape=pltpu.VMEM((2, units, high, LANES), jnp.bfloat16),
        in_specs=[vmem] * 10,
        out_specs=vmem,
        compiler_params=params,
        name="pack",
    )(
        *(
            there(array)
            for array in (
                gain_p,
                gain_f,
                pair_gain_p,
                pair_gain_f,
                hidden_p[0],
                hidden_f[0],
                queries_p[0],
                queries_f[0],
                docs_p,
                docs_f,
            )
        )
    )
    packed = lax.all_to_all(
        packed.reshape(senders, high, LANES), "sp", split_axis=0, concat_axis=0, tiled=True
    )
    far = lax.ppermute(got, "groups", swap)
    pair_keep = lax.ppermute(keep, "fsdp", swap)
    pair_got = lax.ppermute(got, "fsdp", swap)
    pair_far = lax.ppermute(far, "fsdp", swap)
    packed = here(packed)
    parts = pl.pallas_call(
        functools.partial(partial_kernel, tokens),
        out_shape=[pltpu.VMEM((length, 2 * HEAD_DIM), jnp.float32)] * units,
        in_specs=[vmem] * 7,
        out_specs=[vmem] * units,
        scratch_shapes=[pltpu.VMEM((units, length, HEAD_DIM), jnp.float32)] * 2,
        compiler_params=params,
        name="partial",
    )(packed, *(here(array) for array in (keep, got, far, pair_keep, pair_got, pair_far)))
    arrived = [parts[0]]
    for flip in range(1, units):
        arrived.append(
            lax.ppermute(parts[flip], "sp", [(i, i ^ flip) for i in range(senders)])
        )
    cosines, sines = rotary_tables(length)
    mixed = pl.pallas_call(
        functools.partial(attend_kernel, tokens),
        out_shape=pltpu.VMEM((senders, tokens, per_head), jnp.bfloat16),
        in_specs=[vmem] * (3 + units),
        out_specs=vmem,
        compiler_params=params,
        name="attend",
    )(packed, cosines, sines, *(here(part) for part in arrived))
    mixed = lax.all_to_all(mixed, "sp", split_axis=0, concat_axis=0, tiled=True)
    out_shape = jax.ShapeDtypeStruct((tokens, units * per_head), jnp.bfloat16)
    mixed_p, mixed_f = pl.pallas_call(
        assemble_kernel,
        out_shape=[out_shape] * 2,
        in_specs=[vmem],
        out_specs=[vmem] * 2,
        compiler_params=params,
        name="assemble",
    )(here(mixed.reshape(2, units, tokens, per_head)))
    return (mixed_p[None], mixed_f[None])


def per_device(groups, sp_size, fsdp_size, *arrays):
    policy, frozen = arrays[:6], arrays[6:]
    key_heads = policy[4].shape[1] // HEAD_DIM
    tokens = policy[0].shape[1]
    rows = policy[4].shape[0]
    if (
        sp_size == 2 * key_heads
        and key_heads & (key_heads - 1) == 0
        and groups == 2
        and fsdp_size == 2
        and tokens % 16 == 0
        and tokens <= LANES
        and rows % (2 * LANES) == 0
        and SIDE_GAINS + 2 * rows // LANES <= SIDE_ROWS
        and sp_size * tokens <= 512
    ):
        return halves_contract(key_heads, policy, frozen)
    return gathered_weights(policy, frozen)


def solution(mesh):
    return jax.shard_map(
        functools.partial(per_device, *(mesh.shape[axis] for axis in ("groups", "sp", "fsdp"))),
        mesh=mesh,
        in_specs=(
            P(("groups", "fsdp"), "sp", None),
            P(("groups", "fsdp"), "sp", None),
            P(("groups", "fsdp"), "sp"),
            P(("sp", "fsdp")),
            P(("sp", "fsdp"), None),
            P(("sp", "fsdp"), None),
            P(("groups", "fsdp"), "sp", None),
            P(("groups", "fsdp"), "sp", None),
            P(("groups", "fsdp"), "sp"),
            P(("sp", "fsdp")),
            P(("sp", "fsdp"), None),
            P(("sp", "fsdp"), None),
        ),
        out_specs=(P(("groups", "fsdp"), "sp", None), P(("groups", "fsdp"), "sp", None)),
        check_vma=False,
    )
```

```python
import functools

import jax
import jax.numpy as jnp
from jax import lax
from jax.experimental import pallas as pl
from jax.experimental.pallas import tpu as pltpu
from jax.sharding import PartitionSpec as P


HEAD_DIM = 128


EPS = 1e-05
ROPE_BASE = 500000.0
MASKED = -1e30
LANES = 128
SIDE_ROWS = 8
SIDE_GAINS = 4
KERNEL_BYTES = 16 * 2**20


def rotate(raw_keys, positions):
    half_dim = HEAD_DIM // 2
    frequency = jnp.exp(
        -jnp.log(ROPE_BASE) * jnp.arange(half_dim, dtype=jnp.float32) * 2.0 / HEAD_DIM
    )
    angles = positions.astype(jnp.float32)[:, None] * frequency[None, :]
    cosines = jnp.cos(angles)[:, None, :]
    sines = jnp.sin(angles)[:, None, :]
    front_half = raw_keys[..., :half_dim]
    back_half = raw_keys[..., half_dim:]
    return jnp.concatenate(
        [front_half * cosines - back_half * sines, back_half * cosines + front_half * sines],
        axis=-1,
    )


def project(hidden, gain, key_weight, value_weight):
    tokens = hidden.shape[1]
    widened = hidden[0].astype(jnp.float32)
    inverse = lax.rsqrt(jnp.mean(widened * widened, axis=-1, keepdims=True) + EPS)
    scaled = widened * inverse
    gain_rows = lax.all_gather(gain, ("sp", "fsdp"), axis=0, tiled=True)
    key_rows = lax.all_gather(key_weight, ("sp", "fsdp"), axis=0, tiled=True)
    value_rows = lax.all_gather(value_weight, ("sp", "fsdp"), axis=0, tiled=True)
    normed = (scaled * gain_rows.astype(jnp.float32)[None, :]).astype(jnp.bfloat16)
    raw_keys = jnp.dot(normed, key_rows, preferred_element_type=jnp.float32)
    raw_values = jnp.dot(normed, value_rows, preferred_element_type=jnp.float32)
    positions = lax.axis_index("sp") * tokens + jnp.arange(tokens, dtype=jnp.int32)
    key_heads = rotate(raw_keys.reshape(tokens, -1, HEAD_DIM), positions).astype(jnp.bfloat16)
    value_heads = raw_values.astype(jnp.bfloat16).reshape(tokens, -1, HEAD_DIM)
    return (key_heads, value_heads)


def attend(queries, key_heads, value_heads, documents):
    length = queries.shape[0]
    head_count = queries.shape[1]
    block_rows = min(512, length)
    margin = min(512, length // 2)
    window = block_rows + margin
    factor = HEAD_DIM ** (-0.5)
    offsets = jnp.arange(block_rows, dtype=jnp.int32)
    window_offsets = jnp.arange(window, dtype=jnp.int32)
    padding = jnp.zeros((margin, head_count, HEAD_DIM), jnp.bfloat16)
    padded_keys = jnp.concatenate([padding, key_heads], axis=0)
    padded_values = jnp.concatenate([padding, value_heads], axis=0)
    padded_docs = jnp.concatenate([jnp.full((margin,), -1, jnp.int32), documents], axis=0)

    def one_block(block_index):
        first = block_index * block_rows
        query_block = lax.dynamic_slice_in_dim(queries, first, block_rows, 0)
        query_docs = lax.dynamic_slice_in_dim(documents, first, block_rows, 0)
        query_positions = first + offsets
        key_block = lax.dynamic_slice_in_dim(padded_keys, first, window, 0)
        value_block = lax.dynamic_slice_in_dim(padded_values, first, window, 0)
        key_docs = lax.dynamic_slice_in_dim(padded_docs, first, window, 0)
        key_positions = first - margin + window_offsets
        allowed = (key_positions[None, :] <= query_positions[:, None]) & (
            key_docs[None, :] == query_docs[:, None]
        )
        scores = (
            jnp.einsum("qnd,knd->nqk", query_block, key_block, preferred_element_type=jnp.float32)
            * factor
        )
        scores = jnp.where(allowed[None], scores, MASKED)
        highest = jnp.max(scores, axis=-1, keepdims=True)
        exponent = jnp.where(allowed[None], jnp.exp(scores - highest), 0.0)
        weights = (exponent / jnp.sum(exponent, axis=-1, keepdims=True)).astype(jnp.bfloat16)
        blended = jnp.einsum(
            "nqk,knd->qnd", weights, value_block, preferred_element_type=jnp.float32
        )
        return blended.astype(jnp.bfloat16)

    blocks = lax.map(one_block, jnp.arange(length // block_rows, dtype=jnp.int32))
    return blocks.reshape(length, head_count, HEAD_DIM)


def run_model(hidden, queries, documents, gain, key_weight, value_weight):
    tokens = hidden.shape[1]
    head_count = queries.shape[2] // HEAD_DIM
    query_local = queries[0].reshape(tokens, head_count, HEAD_DIM)
    every_doc = lax.all_gather(documents[0], "sp", axis=0, tiled=True)
    key_heads, value_heads = project(hidden, gain, key_weight, value_weight)
    group_size = head_count // key_heads.shape[1]
    wide_keys = jnp.repeat(key_heads, group_size, axis=1)
    wide_values = jnp.repeat(value_heads, group_size, axis=1)
    query_spread, key_spread, value_spread = (
        lax.all_to_all(query_local, "sp", split_axis=1, concat_axis=0, tiled=True),
        lax.all_to_all(wide_keys, "sp", split_axis=1, concat_axis=0, tiled=True),
        lax.all_to_all(wide_values, "sp", split_axis=1, concat_axis=0, tiled=True),
    )
    mixed = attend(query_spread, key_spread, value_spread, every_doc)
    returned = lax.all_to_all(mixed, "sp", split_axis=0, concat_axis=1, tiled=True)
    return returned.reshape(1, tokens, head_count * HEAD_DIM)


def gathered_weights(policy, frozen):
    return (run_model(*policy), run_model(*frozen))


def weights_kernel(key_p, value_p, key_f, value_f, send, keep, sems):
    width = key_p.shape[1]
    model = lax.axis_index("sp") % 2

    def move(key_own, value_own, key_other, value_other):
        copies = [
            pltpu.make_async_copy(source, target, sems.at[index])
            for index, (source, target) in enumerate(
                (
                    (key_other, send.at[:, :width]),
                    (value_other, send.at[:, width:]),
                    (key_own, keep.at[:, :width]),
                    (value_own, keep.at[:, width:]),
                )
            )
        ]
        for copy in copies:
            copy.start()
        for copy in copies:
            copy.wait()

    @pl.when(model == 0)
    def _():
        move(key_p, value_p, key_f, value_f)

    @pl.when(model != 0)
    def _():
        move(key_f, value_f, key_p, value_p)


def pack_kernel(
    gain_p,
    gain_f,
    pair_gain_p,
    pair_gain_f,
    hidden_p,
    hidden_f,
    queries_p,
    queries_f,
    docs_p,
    docs_f,
    *outs_and_scratch,
):
    outs, out = outs_and_scratch[:-1], outs_and_scratch[-1]
    _, units, _, _ = out.shape
    tokens, depth = hidden_p.shape
    rows = gain_p.shape[0]
    block = 2 * rows
    tiles = block // LANES
    per_head = queries_p.shape[1] // units
    row = lax.broadcasted_iota(jnp.int32, (SIDE_ROWS, LANES), 0)
    diagonal = lax.broadcasted_iota(jnp.int32, (tokens, LANES), 0) == lax.broadcasted_iota(
        jnp.int32, (tokens, LANES), 1
    )

    def turned(column):
        return jnp.sum(jnp.where(diagonal, column, 0.0), axis=0, keepdims=True)

    for owner, (hidden, queries, docs, gain, pair_gain) in enumerate(
        (
            (hidden_p, queries_p, docs_p, gain_p, pair_gain_p),
            (hidden_f, queries_f, docs_f, gain_f, pair_gain_f),
        )
    ):
        widened = hidden[...].astype(jnp.float32)
        mean = jnp.sum(widened * widened, axis=-1, keepdims=True) * (1.0 / depth)
        inverse = lax.rsqrt(mean + EPS)
        high = inverse.astype(jnp.bfloat16).astype(jnp.float32)
        middle = (inverse - high).astype(jnp.bfloat16).astype(jnp.float32)
        low = inverse - high - middle
        doc = jnp.concatenate(
            [docs[...].astype(jnp.float32), jnp.zeros((1, LANES - tokens), jnp.float32)], axis=-1
        )
        gains = [gain[...].reshape(1, rows).astype(jnp.float32)]
        gains.append(pair_gain[...].reshape(1, rows).astype(jnp.float32))
        side = jnp.where(row == 0, turned(high), 0.0)
        side = jnp.where(row == 1, turned(middle), side)
        side = jnp.where(row == 2, turned(low), side)
        side = jnp.where(row == 3, doc, side)
        for which in range(2):
            for part in range(rows // LANES):
                side = jnp.where(
                    row == SIDE_GAINS + which * (rows // LANES) + part,
                    gains[which][:, part * LANES : (part + 1) * LANES],
                    side,
                )
        side = side.astype(jnp.bfloat16)
        for unit in range(units):
            for tile in range(2 * tiles):
                first = (2 * tiles * unit + tile) * LANES
                out[owner, unit, tile * tokens : (tile + 1) * tokens, :] = hidden[
                    :, first : first + LANES
                ]
            for tile in range(per_head // LANES):
                first = unit * per_head + tile * LANES
                low = (2 * tiles + tile) * tokens
                out[owner, unit, low : low + tokens, :] = queries[:, first : first + LANES]
            out[owner, unit, out.shape[2] - SIDE_ROWS :, :] = side
    place = lax.axis_index("sp")
    for flip in range(2 * units):
        outs[flip][...] = out[(place ^ flip) % 2, (place ^ flip) // 2]


def side_columns(side, tokens, sums):
    senders = side.shape[0]
    turned = jnp.transpose(side.reshape(senders * SIDE_ROWS, LANES))
    columns = []
    for sender in range(senders):
        column = None
        for index in sums:
            first = sender * SIDE_ROWS + index
            part = turned[:tokens, first : first + 1]
            column = part if column is None else column + part
        columns.append(column)
    return jnp.concatenate(columns, axis=0)


def partial_kernel(tokens, units, *refs):
    chunks, (own, other), refs = refs[:units], refs[units : units + 2], refs[units + 2 :]
    keep, got, pair_keep, pair_got = refs[:4]
    outs, (packed, keys, values) = refs[4 : 4 + units], refs[4 + units :]
    place, core = lax.axis_index("sp"), lax.axis_index("fsdp")
    plane, model = place // 2, place % 2
    high = packed.shape[1]
    length = units * tokens
    rows = keep.shape[0]
    width = keep.shape[1] // 2
    strips = rows // LANES
    for flip in range(units):
        packed[(place % units) ^ flip] = chunks[flip][...]
    side_row = high - SIDE_ROWS
    inverse = side_columns(packed[:, side_row:, :].astype(jnp.float32), tokens, (0, 1, 2))
    own_side = own[side_row:, :].astype(jnp.float32)
    other_side = other[side_row:, :].astype(jnp.float32)
    key_sum = value_sum = None
    for weights, flip_model, flip_core in (
        (keep, 0, 0),
        (pair_keep, 0, 1),
        (got, 1, 0),
        (pair_got, 1, 1),
    ):
        side = other_side if flip_model else own_side
        columns = []
        for strip in range(strips):
            tile = ((model ^ flip_model) * 2 + (core ^ flip_core)) * strips + strip
            hidden = packed[:, pl.ds(pl.multiple_of(tile * tokens, tokens), tokens), :]
            hidden = hidden.reshape(length, LANES).astype(jnp.float32)
            wanted = SIDE_GAINS + flip_core * strips + strip
            gain = side[wanted : wanted + 1, :]
            columns.append((hidden * inverse * gain).astype(jnp.bfloat16))
        normed = jnp.concatenate(columns, axis=-1)
        key_part = jnp.dot(normed, weights[:, :width], preferred_element_type=jnp.float32)
        value_part = jnp.dot(normed, weights[:, width:], preferred_element_type=jnp.float32)
        key_sum = key_part if key_sum is None else key_sum + key_part
        value_sum = value_part if value_sum is None else value_sum + value_part
    for head in range(units):
        keys[head] = key_sum[:, head * HEAD_DIM : (head + 1) * HEAD_DIM]
        values[head] = value_sum[:, head * HEAD_DIM : (head + 1) * HEAD_DIM]
    for flip in range(units):
        outs[flip][:, :HEAD_DIM] = keys[plane ^ flip]
        outs[flip][:, HEAD_DIM:] = values[plane ^ flip]


def add_kernel(left, right, out):
    out[...] = left[...] + right[...]


def attend_kernel(tokens, units, cosines, sines, *refs):
    chunks, refs = refs[: 2 * units], refs[2 * units :]
    near, far, refs = refs[:3], refs[3:6], refs[6:]
    out, asked, side, total = refs
    senders, _, per_head = out.shape
    length = senders * tokens
    place = lax.axis_index("sp")
    half = place // units
    high = chunks[0].shape[0]
    first_query = high - SIDE_ROWS - per_head // HEAD_DIM * tokens
    for flip in range(senders):
        asked[place ^ flip] = chunks[flip][first_query : high - SIDE_ROWS, :]
        side[place ^ flip] = chunks[flip][high - SIDE_ROWS :, :].astype(jnp.float32)
    for which, parts in ((half, near), (1 - half, far)):
        part_sum = parts[0][...]
        for part in parts[1:]:
            part_sum = part_sum + part[...]
        total[which] = part_sum
    sums = total[...].reshape(length, 2 * HEAD_DIM)
    raw_keys = sums[:, :HEAD_DIM]
    turned = jnp.concatenate(
        [raw_keys[:, HEAD_DIM // 2 :], raw_keys[:, : HEAD_DIM // 2]], axis=-1
    )
    keys = (raw_keys * cosines[...] + turned * sines[...]).astype(jnp.bfloat16)
    values = sums[:, HEAD_DIM:].astype(jnp.bfloat16)
    query_docs = side_columns(side[...], tokens, (3,))
    key_docs = jnp.transpose(jnp.broadcast_to(query_docs, (length, LANES)))[:1, :]
    row = lax.broadcasted_iota(jnp.int32, (length, length), 0)
    column = lax.broadcasted_iota(jnp.int32, (length, length), 1)
    allowed = (column <= row) & (query_docs == key_docs)
    for head in range(per_head // HEAD_DIM):
        queries = asked[:, head * tokens : (head + 1) * tokens, :].reshape(length, HEAD_DIM)
        scores = lax.dot_general(
            queries, keys, (((1,), (1,)), ((), ())), preferred_element_type=jnp.float32
        ) * (HEAD_DIM ** (-0.5))
        scores = jnp.where(allowed, scores, MASKED)
        highest = jnp.max(scores, axis=-1, keepdims=True)
        exponent = jnp.where(allowed, jnp.exp(scores - highest), 0.0)
        weights = (exponent / jnp.sum(exponent, axis=-1, keepdims=True)).astype(jnp.bfloat16)
        mixed = jnp.dot(weights, values, preferred_element_type=jnp.float32)
        out[:, :, head * HEAD_DIM : (head + 1) * HEAD_DIM] = mixed.astype(jnp.bfloat16).reshape(
            senders, tokens, HEAD_DIM
        )


def assemble_kernel(arrived, out_p, out_f):
    senders, _, per_head = arrived.shape
    for sender in range(senders):
        out = (out_p, out_f)[sender % 2]
        head = sender // 2
        out[:, head * per_head : (head + 1) * per_head] = arrived[sender]


def here(x):
    return pltpu.with_memory_space_constraint(x, pltpu.VMEM)


def there(x):
    return pltpu.with_memory_space_constraint(x, pltpu.HBM)


def rotary_tables(length):
    half_dim = HEAD_DIM // 2
    frequency = jnp.exp(
        -jnp.log(ROPE_BASE) * jnp.arange(half_dim, dtype=jnp.float32) * 2.0 / HEAD_DIM
    )
    angles = jnp.arange(length, dtype=jnp.int32).astype(jnp.float32)[:, None] * frequency[None, :]
    cosines, sines = jnp.cos(angles), jnp.sin(angles)
    return (
        jnp.concatenate([cosines, cosines], axis=-1),
        jnp.concatenate([-sines, sines], axis=-1),
    )


def planes_contract(units, policy, frozen):
    hidden_p, queries_p, docs_p, gain_p, key_p, value_p = policy
    hidden_f, queries_f, docs_f, gain_f, key_f, value_f = frozen
    tokens = hidden_p.shape[1]
    rows, width = key_p.shape
    per_head = queries_p.shape[2] // units
    senders = 2 * units
    length = senders * tokens
    high = (4 * rows + per_head) // LANES * tokens + SIDE_ROWS
    vmem = pl.BlockSpec(memory_space=pltpu.VMEM)
    hbm = pl.BlockSpec(memory_space=pltpu.HBM)
    params = pltpu.CompilerParams(vmem_limit_bytes=KERNEL_BYTES)
    swap = [(0, 1), (1, 0)]

    def flipped(flip):
        return [(i, i ^ flip) for i in range(senders)]

    send, keep = pl.pallas_call(
        weights_kernel,
        out_shape=[
            pltpu.VMEM((rows, 2 * width), jnp.bfloat16),
            pltpu.VMEM((rows, 2 * width), jnp.bfloat16),
        ],
        in_specs=[hbm] * 4,
        out_specs=[vmem] * 2,
        scratch_shapes=[pltpu.SemaphoreType.DMA((4,))],
        compiler_params=params,
        name="weights",
    )(*(there(array) for array in (key_p, value_p, key_f, value_f)))
    got = lax.ppermute(send, "sp", flipped(1))
    pair_gain_p = lax.ppermute(gain_p, "fsdp", swap)
    pair_gain_f = lax.ppermute(gain_f, "fsdp", swap)
    sent = pl.pallas_call(
        pack_kernel,
        out_shape=[pltpu.VMEM((high, LANES), jnp.bfloat16)] * senders,
        in_specs=[vmem] * 10,
        out_specs=[vmem] * senders,
        scratch_shapes=[pltpu.VMEM((2, units, high, LANES), jnp.bfloat16)],
        compiler_params=params,
        name="pack",
    )(
        *(
            there(array)
            for array in (
                gain_p,
                gain_f,
                pair_gain_p,
                pair_gain_f,
                hidden_p[0],
                hidden_f[0],
                queries_p[0],
                queries_f[0],
                docs_p,
                docs_f,
            )
        )
    )
    chunks = [sent[0]]
    for flip in range(1, senders):
        chunks.append(lax.ppermute(sent[flip], "sp", flipped(flip)))
    pair_keep = lax.ppermute(keep, "fsdp", swap)
    pair_got = lax.ppermute(got, "fsdp", swap)
    chunks = [here(chunk) for chunk in chunks]
    weights = [here(array) for array in (keep, got, pair_keep, pair_got)]
    block = pltpu.VMEM((units * tokens, 2 * HEAD_DIM), jnp.float32)
    sums, crossed = {}, {}
    for side in ("near", "far"):
        first = units if side == "far" else 0
        own, local, hold, cross = pl.pallas_call(
            functools.partial(partial_kernel, tokens, units),
            out_shape=[block] * units,
            in_specs=[vmem] * (units + 6),
            out_specs=[vmem] * units,
            scratch_shapes=[
                pltpu.VMEM((units, high, LANES), jnp.bfloat16),
                pltpu.VMEM((units, units * tokens, HEAD_DIM), jnp.float32),
                pltpu.VMEM((units, units * tokens, HEAD_DIM), jnp.float32),
            ],
            compiler_params=params,
        )(*chunks[first : first + units], chunks[0], chunks[1], *weights)
        cross = lax.ppermute(cross, "sp", flipped(2))
        local = lax.ppermute(local, "sp", flipped(2))
        both = pl.pallas_call(
            add_kernel, out_shape=block, in_specs=[vmem] * 2, out_specs=vmem, compiler_params=params
        )(here(hold), here(cross))
        crossed[side] = lax.ppermute(both, "sp", flipped(4))
        sums[side] = [own, local]
    arrived = [
        here(part)
        for part in (*sums["near"], crossed["far"], *sums["far"], crossed["near"])
    ]
    cosines, sines = rotary_tables(length)
    mixed = pl.pallas_call(
        functools.partial(attend_kernel, tokens, units),
        out_shape=pltpu.VMEM((senders, tokens, per_head), jnp.bfloat16),
        in_specs=[vmem] * (2 + senders + len(arrived)),
        out_specs=vmem,
        scratch_shapes=[
            pltpu.VMEM((senders, per_head // HEAD_DIM * tokens, HEAD_DIM), jnp.bfloat16),
            pltpu.VMEM((senders, SIDE_ROWS, LANES), jnp.float32),
            pltpu.VMEM((2, units * tokens, 2 * HEAD_DIM), jnp.float32),
        ],
        compiler_params=params,
        name="attend",
    )(cosines, sines, *chunks, *arrived)
    mixed = lax.all_to_all(mixed, "sp", split_axis=0, concat_axis=0, tiled=True)
    out_shape = jax.ShapeDtypeStruct((tokens, units * per_head), jnp.bfloat16)
    mixed_p, mixed_f = pl.pallas_call(
        assemble_kernel,
        out_shape=[out_shape] * 2,
        in_specs=[vmem],
        out_specs=[vmem] * 2,
        compiler_params=params,
        name="assemble",
    )(here(mixed))
    return (mixed_p[None], mixed_f[None])


def per_device(sp_size, fsdp_size, *arrays):
    policy, frozen = arrays[:6], arrays[6:]
    key_heads = policy[4].shape[1] // HEAD_DIM
    tokens = policy[0].shape[1]
    rows = policy[4].shape[0]
    if (
        sp_size == 8
        and key_heads == 4
        and fsdp_size == 2
        and tokens % 16 == 0
        and tokens <= LANES
        and rows % LANES == 0
        and SIDE_GAINS + 2 * rows // LANES <= SIDE_ROWS
        and sp_size * tokens <= 512
    ):
        return planes_contract(key_heads, policy, frozen)
    return gathered_weights(policy, frozen)


def solution(mesh):
    return jax.shard_map(
        functools.partial(per_device, *(mesh.shape[axis] for axis in ("sp", "fsdp"))),
        mesh=mesh,
        in_specs=(
            P(("groups", "fsdp"), "sp", None),
            P(("groups", "fsdp"), "sp", None),
            P(("groups", "fsdp"), "sp"),
            P(("sp", "fsdp")),
            P(("sp", "fsdp"), None),
            P(("sp", "fsdp"), None),
            P(("groups", "fsdp"), "sp", None),
            P(("groups", "fsdp"), "sp", None),
            P(("groups", "fsdp"), "sp"),
            P(("sp", "fsdp")),
            P(("sp", "fsdp"), None),
            P(("sp", "fsdp"), None),
        ),
        out_specs=(P(("groups", "fsdp"), "sp", None), P(("groups", "fsdp"), "sp", None)),
        check_vma=False,
    )
```
